256 devices in a mesh: ctx: 32 (over z, y), head: 8 (over x, core).
Axes of the slice: x: 4, y: 4, z: 8, core: 2. Of those that a mesh axis runs over, the one named last changes fastest.
Arguments:
- query: bfloat16 [32, 128, 576], P('ctx', 'head'), may hold values from -20 to 20
- cache: bfloat16 [131072, 576], P('ctx'), may hold values from -20 to 20
- cotangent: bfloat16 [32, 128, 512], P('ctx', 'head'), may hold values from -6 to 6
- positions: int32 [32], P('ctx'), may hold values from 0 to 262143
- visible: int32 [32], replicated, may hold values from 128 to 131072, as said below
Outputs:
- attention: bfloat16 [32, 128, 512], P('ctx', 'head')
- grad_query: float32 [32, 128, 576], P('ctx', 'head')
- grad_cache: bfloat16 [131072, 576], P('ctx')
The draws below stay inside these ranges and needn't reach their ends.
Inputs may be any that keep to these rules, and one draw needn't show every extreme that they name: `visible`: each entry is a multiple of 128; some rollout token sees all 131072 prompt tokens.
All inputs are finite; a program needn't handle non-finite values.
Results may differ from the reference program's by a relative error of at most 0.01855.
Values may be sent and summed in bfloat16 or wider, within the bound.
A program may use at most 128 MiB of HBM per device.

```python
import jax
import jax.numpy as jnp
import numpy as np
from jax import lax

VDIM = 512
RDIM = 64
BLOCK = 128
HEADS = 128
TOKENS = 32
PROMPT = 131072


def planted_row(key):
    amplitude = (160.0 * 192.0 ** 0.5 / VDIM) ** 0.5
    sign_bits = jax.random.bernoulli(jax.random.fold_in(key, 91), 0.5, (VDIM,))
    return jnp.where(sign_bits, amplitude, -amplitude).astype(jnp.float32)


def draw_query(key, part):
    full_shape = (TOKENS, HEADS, VDIM + RDIM)
    drawn = jnp.clip(jax.random.normal(jax.random.fold_in(key, 1), full_shape), -4.0, 4.0)
    planted = planted_row(key)
    padding = jnp.zeros((RDIM,), jnp.float32)
    strengths = [0.7, 1.0, 1.5]
    head_slots = [0, HEADS // 2, HEADS - 1]
    for slot_index in range(3):
        planted_query = jnp.concatenate([strengths[slot_index] * planted, padding])
        drawn = drawn.at[slot_index, head_slots[slot_index]].set(planted_query)
    return drawn.astype(jnp.bfloat16)


def draw_cache(key, part):
    full_shape = (PROMPT, VDIM + RDIM)
    drawn = jnp.clip(jax.random.normal(jax.random.fold_in(key, 3), full_shape), -4.0, 4.0)
    planted = planted_row(key)
    alternate = jnp.where(jnp.arange(VDIM) % 2 == 0, 0.5, -0.5)
    second = planted * (0.9875 + alternate)
    padding = jnp.zeros((RDIM,), jnp.float32)
    drawn = drawn.at[0].set(jnp.concatenate([planted, padding]))
    drawn = drawn.at[1].set(jnp.concatenate([second, padding]))
    return drawn.astype(jnp.bfloat16)


def draw_visible(key, part):
    blocks = PROMPT // BLOCK
    counts = jax.random.randint(jax.random.fold_in(key, 5), (TOKENS,), 1, blocks + 1)
    chosen = jax.random.randint(jax.random.fold_in(key, 6), (), 0, TOKENS)
    counts = jnp.where(jnp.arange(TOKENS) == chosen, blocks, counts)
    return (counts * BLOCK).astype(jnp.int32)


def place_ends(values, own_key, low, top_value):
    shape = values.shape
    index_at = [jax.random.randint(jax.random.fold_in(own_key, axis), (), 0, shape[axis]) for axis in range(len(shape))]
    values = values.at[tuple(index_at)].set(low)
    longest = shape.index(max(shape))
    index_at[longest] = (index_at[longest] + 1) % shape[longest]
    return values.at[tuple(index_at)].set(top_value)


def levels(stream_key, shape, cuts, low, high):
    loudness, own = 1.0, jax.random.fold_in(stream_key, 6)
    for position, blocks in cuts:
        heights = jnp.exp(jax.random.uniform(jax.random.fold_in(own, position), (blocks,), jnp.float32, low / len(cuts), high / len(cuts)))
        loudness = loudness * jnp.repeat(heights, shape[position] // blocks).reshape([-1 if axis == position else 1 for axis in range(len(shape))])
    return loudness


def normal_values(own_key, dims, width, most, split=(), held_as=jnp.bfloat16):
    gain = levels(own_key, dims, split, -0.22, 0.18) if split else 1.0
    values = jax.random.normal(own_key, dims, jnp.float32) * width * gain
    return jnp.minimum(jnp.maximum(values, -most), most).astype(held_as)


def setup_inputs(seed: int = 0) -> dict:
    keys = jax.random.split(jax.random.key(seed), 6)
    return {
        "query": draw_query(jax.random.fold_in(keys[5], 71), 0),
        "cache": draw_cache(jax.random.fold_in(keys[5], 71), 0),
        "cotangent": normal_values(keys[2], (TOKENS, HEADS, VDIM), 1.0, 6.0, ((0, 32), (1, 8))),
        "positions": place_ends(jax.random.randint(keys[3], (TOKENS,), 0, 262144), jax.random.fold_in(keys[3], 1), 0, 262143).astype(jnp.int32),
        "visible": draw_visible(jax.random.fold_in(keys[5], 71), 0),
    }


softmax_scale = 192.0 ** -0.5
position_bits = 18
masked_value = -1.0e30


def rotation(positions, half_width):
    frequency = 10000.0 ** (-np.arange(half_width) / half_width)
    angles = np.outer(2.0 ** np.arange(position_bits), frequency)
    cosine_table = jnp.asarray(np.cos(angles), jnp.float32)
    sine_table = jnp.asarray(np.sin(angles), jnp.float32)
    cosines = jnp.ones((positions.shape[0], half_width), jnp.float32)
    sine_part = jnp.zeros((positions.shape[0], half_width), jnp.float32)
    for bit_index in range(position_bits):
        switch = ((positions // (2 ** bit_index)) % 2).astype(jnp.float32)[:, None]
        step_cos = 1.0 + switch * (cosine_table[bit_index] - 1.0)
        step_sin = switch * sine_table[bit_index]
        cosines, sine_part = cosines * step_cos - sine_part * step_sin, sine_part * step_cos + cosines * step_sin
    return cosines[:, None, :], sine_part[:, None, :]


def rotate(tensor, cosines, sine_part, value_width, inverse):
    half_width = cosines.shape[-1]
    lower = tensor[..., value_width:value_width + half_width]
    upper = tensor[..., value_width + half_width:]
    if inverse:
        sine_part = -sine_part
    new_lower = lower * cosines - upper * sine_part
    new_upper = lower * sine_part + upper * cosines
    return jnp.concatenate([tensor[..., :value_width], new_lower, new_upper], axis=-1)


def reference(query, cache, cotangent, positions, visible):
    value_width = cotangent.shape[-1]
    half_width = (query.shape[-1] - value_width) // 2
    cosines, sine_part = rotation(positions, half_width)
    rotated = rotate(query.astype(jnp.float32), cosines, sine_part, value_width, False).astype(jnp.bfloat16)
    allowed = jnp.arange(cache.shape[0]).astype(jnp.int32)[None, :] < visible[:, None]
    values = cache[:, :value_width]
    extra_width = cache.shape[1] - value_width

    def per_head(carry, inputs):
        query_head, grad_head = inputs
        scores = jnp.dot(query_head, cache.T, preferred_element_type=jnp.float32) * softmax_scale
        scores = jnp.where(allowed, scores, masked_value)
        peak = jnp.max(scores, axis=1, keepdims=True)
        weights = jnp.where(allowed, jnp.exp(scores - peak), 0.0)
        totals = jnp.sum(weights, axis=1, keepdims=True)
        probs = weights / totals
        prob_low = probs.astype(jnp.bfloat16)
        attended = jnp.dot(prob_low, values, preferred_element_type=jnp.float32)
        grad_probs = jnp.dot(grad_head, values.T, preferred_element_type=jnp.float32)
        delta = jnp.sum(grad_head.astype(jnp.float32) * attended, axis=1, keepdims=True)
        grad_scores = (probs * (grad_probs - delta) * softmax_scale).astype(jnp.bfloat16)
        grad_rotated = jnp.dot(grad_scores, cache, preferred_element_type=jnp.float32)
        grad_latent = jnp.dot(grad_scores.T, query_head, preferred_element_type=jnp.float32)
        grad_value = jnp.dot(prob_low.T, grad_head, preferred_element_type=jnp.float32)
        grad_latent = grad_latent + jnp.pad(grad_value, ((0, 0), (0, extra_width)))
        return carry + grad_latent, (attended, grad_rotated)

    start = jnp.zeros(cache.shape, jnp.float32)
    summed, (attended, grad_rotated) = lax.scan(per_head, start, (jnp.swapaxes(rotated, 0, 1), jnp.swapaxes(cotangent, 0, 1)))
    attention = jnp.swapaxes(attended, 0, 1).astype(jnp.bfloat16)
    grad_query = rotate(jnp.swapaxes(grad_rotated, 0, 1), cosines, sine_part, value_width, True)
    return attention, grad_query, summed.astype(jnp.bfloat16)
```

```python
import jax
import jax.numpy as jnp
import numpy as np
from jax import lax
from jax.experimental import pallas as pl
from jax.experimental.pallas import tpu as pltpu
from jax.sharding import PartitionSpec as P

softmax_scale = 192.0 ** (-0.5)
log2_scale = softmax_scale * float(np.log2(np.e))
position_bits = 18
masked_value = -1e30

SZ, SY, SX = 8, 4, 4
CTX, HEAD = SZ * SY, SX * 2
F32, BF16 = jnp.float32, jnp.bfloat16
MESH = pl.DeviceIdType.MESH


def remote(src, dst, send_sem, recv_sem, device):
    return pltpu.make_async_remote_copy(
        src_ref=src,
        dst_ref=dst,
        send_sem=send_sem,
        recv_sem=recv_sem,
        device_id=device,
        device_id_type=MESH,
    )


def rows8(value, op):
    groups = value.reshape(value.shape[0] // 8, 8, value.shape[1])
    return op(groups, axis=0)


def kernel(
    vis_ref, pos_ref, cos_ref, sin_ref, query_ref, cot_ref, cache_ref,
    att_ref, gq_ref, gc_ref,
    qb, dob, keys, keys_t, q_t, do_t, qdo, scores, gprobs, low, grads,
    stat_own, stat_y, stat_z, acc, dd_out, dd_in, opp_out, opp_in, rs_out, rs_in,
    att_out, att_in, gq_out, gq_in,
    cache_sem, qy_s, qy_r, qz_s, qz_r, dz_s, dz_r, dy_s, dy_r,
    sy_s, sy_r, sz_s, sz_r, dd_s, dd_r, op_s, op_r, rs_s, rs_r,
    ag_s, ag_r, fw_s, fw_r, pp_s, pp_r, out_sem, at_s, at_r, gq_s, gq_r,
):
    ctx = lax.axis_index("ctx")
    head = lax.axis_index("head")
    z, y = ctx // SY, ctx % SY
    x, core = head // 2, head % 2
    n_keys = keys.shape[0]
    vd = cot_ref.shape[1]
    width = query_ref.shape[1]
    per = query_ref.shape[0]
    rows = CTX * per
    own_keys = n_keys // HEAD
    wave_keys = own_keys // 2
    half_keys = wave_keys // 2
    sends = []

    def plane(zz, yy):
        return (zz % SZ) * SY + yy % SY, head

    right = (ctx, ((x + 1) % SX) * 2 + core)
    left = (ctx, ((x + SX - 1) % SX) * 2 + core)
    partner = (ctx, x * 2 + 1 - core)

    def send(*args):
        copy = remote(*args)
        copy.start()
        sends.append(copy)

    def arrive(dst, send_sem, recv_sem, device):
        remote(dst, dst, send_sem, recv_sem, device).wait_recv()

    load = pltpu.make_async_copy(cache_ref, keys, cache_sem)
    load.start()

    barrier = pltpu.get_barrier_semaphore()

    def greet(k, carry):
        pl.semaphore_signal(
            barrier, inc=1, device_id=((ctx + k) % CTX, head), device_id_type=MESH
        )
        return carry

    lax.fori_loop(1, CTX, greet, 0)
    for device in (right, left, partner):
        pl.semaphore_signal(barrier, inc=1, device_id=device, device_id_type=MESH)

    position = pos_ref[0]
    half = (width - vd) // 2
    cosines = jnp.ones((1, 2 * half), F32)
    sines = jnp.zeros((1, 2 * half), F32)
    for bit in range(position_bits):
        switch = ((position >> bit) & 1).astype(F32)
        step_cos = 1.0 + switch * (cos_ref[bit : bit + 1, :] - 1.0)
        step_sin = switch * sin_ref[bit : bit + 1, :]
        cosines, sines = (
            cosines * step_cos - sines * step_sin,
            sines * step_cos + cosines * step_sin,
        )
    lower = lax.broadcasted_iota(jnp.int32, (1, 2 * half), 1) < half
    signed = jnp.where(lower, -sines, sines)

    def swapped(t):
        return jnp.concatenate([t[:, half:], t[:, :half]], axis=1)

    rotary = query_ref[:, vd:].astype(F32)
    qb[z, y, :, :vd] = query_ref[:, :vd]
    qb[z, y, :, vd:] = (rotary * cosines + swapped(rotary) * signed).astype(BF16)
    dob[z, y] = cot_ref[...]

    lane = lax.broadcasted_iota(jnp.int32, (1, rows), 1) // per
    seen = jnp.zeros((1, rows), jnp.int32)
    for t in range(CTX):
        seen = jnp.where(lane == t, vis_ref[t], seen)

    pl.semaphore_wait(barrier, CTX - 1 + 3)

    for d in range(1, SY):
        send(qb.at[z, y], qb.at[z, y], qy_s.at[d], qy_r.at[d], plane(z, y + d))
    for d in range(1, SZ):
        send(dob.at[z, y], dob.at[z, y], dz_s.at[d], dz_r.at[d], plane(z + d, y))

    def ring(way, step, d):
        sign = 1 if way == 0 else -1
        zz = (z - sign * (step - 1) + SZ) % SZ
        yy = (y - d + SY) % SY
        at = (way * (SZ // 2) + step - 1) * SY + d
        block = qb.at[zz, yy]
        send(block, block, qz_s.at[at], qz_r.at[at], plane(z + sign + SZ, y))

    def ring_arrive(way, step, d):
        sign = 1 if way == 0 else -1
        zz = (z - sign * step + SZ) % SZ
        yy = (y - d + SY) % SY
        at = (way * (SZ // 2) + step - 1) * SY + d
        arrive(qb.at[zz, yy], qz_s.at[at], qz_r.at[at], plane(z + sign + SZ, y))

    def carried(way, step, d):
        return step < SZ // 2 or (d < SY // 2) == (way == 0)

    n_t = 8
    t_keys = n_keys // n_t

    def transpose_keys(i):
        at = i * t_keys
        keys_t[:, at : at + t_keys] = keys[at : at + t_keys, :].T

    for d in range(SY):
        if d:
            src = qb.at[z, (y - d + SY) % SY]
            arrive(src, qy_s.at[d], qy_r.at[d], plane(z, y + d))
        ring(0, 1, d)
        ring(1, 1, d)
        if d == 0:
            load.wait()
            transpose_keys(0)
    for step in range(1, SZ // 2 + 1):
        transpose_keys(2 * step - 1)
        if 2 * step < n_t:
            transpose_keys(2 * step)
        for d in range(SY):
            for way in range(2):
                if carried(way, step, d):
                    ring_arrive(way, step, d)
                    if step < SZ // 2 and carried(way, step + 1, d):
                        ring(way, step + 1, d)
        if step == 2:
            for d in range(1, SZ):
                src = dob.at[(z - d + SZ) % SZ, y]
                arrive(src, dz_s.at[d], dz_r.at[d], plane(z + d, y))
            for d in range(1, SY):
                src = dob.at[:, y]
                send(src, src, dy_s.at[d], dy_r.at[d], plane(z, y + d))

    q_all = qb[...].reshape(rows, width)
    q_t[...] = q_all.T
    qdo[:rows, :] = q_all[:, :vd]
    chunk = 256
    n_chunks = n_keys // chunk
    first_key = ctx * n_keys

    def score(i, top):
        at = pl.multiple_of(i * chunk, chunk)
        raw = jnp.dot(keys[pl.ds(at, chunk), :], q_t[...], preferred_element_type=F32)
        base = first_key + at
        for part in range(chunk // 128):
            bias = jnp.where(base + part * 128 < seen, 0.0, masked_value).astype(F32)
            piece = raw[part * 128 : (part + 1) * 128, :] * log2_scale + bias
            scores[pl.ds(pl.multiple_of(at + part * 128, 128), 128), :] = piece
            top = jnp.maximum(top, rows8(piece, jnp.max))
        return top

    top = lax.fori_loop(0, n_chunks, score, jnp.full((8, rows), 2 * masked_value, F32))
    peak = jnp.max(top, axis=0, keepdims=True)

    for d in range(1, SY):
        src = dob.at[:, (y - d + SY) % SY]
        arrive(src, dy_s.at[d], dy_r.at[d], plane(z, y + d))
    do_all = dob[...].reshape(rows, vd)
    do_t[...] = do_all.T
    qdo[rows:, :] = do_all

    def weigh(i, sums):
        mass, inner = sums
        at = pl.multiple_of(i * chunk, chunk)
        window = pl.ds(at, chunk)
        weights = jnp.exp2(scores[window, :] - peak)
        gp = jnp.dot(keys[window, :vd], do_t[...], preferred_element_type=F32)
        scores[window, :] = weights
        gprobs[window, :] = gp
        low[window, :] = weights.astype(BF16)
        return mass + rows8(weights, jnp.sum), inner + rows8(weights * gp, jnp.sum)

    zero = jnp.zeros((8, rows), F32)
    mass, inner = lax.fori_loop(0, n_chunks, weigh, (zero, zero))
    mass = jnp.sum(mass, axis=0, keepdims=True)
    inner = jnp.sum(inner, axis=0, keepdims=True)

    n_lines = rows // 128

    def put_stats(ref, stats):
        for k, stat in enumerate(stats):
            for i in range(n_lines):
                ref[k * n_lines + i : k * n_lines + i + 1, :] = stat[:, i * 128 : (i + 1) * 128]

    def merge(parts):
        tops = [p[:n_lines] for p in parts]
        best = tops[0]
        for t in tops[1:]:
            best = jnp.maximum(best, t)
        total, dots = 0.0, 0.0
        for t, p in zip(tops, parts):
            factor = jnp.exp2(t - best)
            total = total + factor * p[n_lines : 2 * n_lines]
            dots = dots + factor * p[2 * n_lines : 3 * n_lines]
        return best, total, dots

    put_stats(stat_own, (peak, mass, inner, jnp.zeros_like(peak)))
    for d in range(1, SY):
        send(stat_own, stat_y.at[d], sy_s.at[d], sy_r.at[d], plane(z, y + d))
    first = jnp.dot(keys_t[:vd, :], low[:, : rows // 2], preferred_element_type=F32)
    for d in range(1, SY):
        arrive(stat_y.at[d], sy_s.at[d], sy_r.at[d], plane(z, y + d))
    best, total, dots = merge([stat_own[...]] + [stat_y[d] for d in range(1, SY)])
    stat_z[0, :n_lines] = best
    stat_z[0, n_lines : 2 * n_lines] = total
    stat_z[0, 2 * n_lines : 3 * n_lines] = dots
    stat_z[0, 3 * n_lines :] = jnp.zeros_like(dots)
    for d in range(1, SZ):
        send(stat_z.at[0], stat_z.at[d], sz_s.at[d], sz_r.at[d], plane(z + d, y))
    second = jnp.dot(keys_t[:vd, :], low[:, rows // 2 :], preferred_element_type=F32)
    att_t = jnp.concatenate([first, second], axis=1)
    for d in range(1, SZ):
        arrive(stat_z.at[d], sz_s.at[d], sz_r.at[d], plane(z + d, y))
    best, total, dots = merge([stat_z[d] for d in range(SZ)])

    def across(v):
        return jnp.concatenate([v[i : i + 1, :] for i in range(n_lines)], axis=1)

    factor = jnp.exp2(peak - across(best)) / across(total)
    delta = across(dots) / across(total)

    att_out[...] = (att_t * factor).T.astype(BF16).reshape(CTX, per, vd)

    def send_att(k, carry):
        to = (ctx + k) % CTX
        remote(att_out.at[to], att_in.at[k], at_s.at[k], at_r.at[k], (to, head)).start()
        return carry

    lax.fori_loop(1, CTX, send_att, 0)

    def spot(xx, cc, wave):
        return pl.multiple_of((xx * 2 + cc) * own_keys + wave * wave_keys, wave_keys)

    def terms(at):
        window = pl.ds(at, wave_keys)
        probs = scores[window, :] * factor
        grad = (probs * (gprobs[window, :] - delta) * softmax_scale).astype(BF16)
        grads[window, :] = grad
        both = jnp.concatenate([grad, probs.astype(BF16)], axis=1)
        value = jnp.dot(both, qdo[...], preferred_element_type=F32)
        q_rotary = qb[...].reshape(rows, width)[:, vd:]
        return value, jnp.dot(grad, q_rotary, preferred_element_type=F32)

    offsets = (2, 1, 3, 0)
    halves = (slice(0, half_keys), slice(half_keys, 2 * half_keys))

    def chip_sum(wave, slot, part):
        at = wave * 4 + slot
        return acc[at, part, :] + dd_in[at, part, :].astype(F32)

    def start_wave(wave):
        for slot, offset in enumerate(offsets):
            at = wave * 4 + slot
            xx = (x + offset) % SX
            value, rotary_part = terms(spot(xx, 1 - core, wave))
            dd_out[at, :, :vd] = value.astype(BF16)
            dd_out[at, :, vd:] = rotary_part.astype(BF16)
            send(dd_out.at[at], dd_in.at[at], dd_s.at[at], dd_r.at[at], partner)
            value, rotary_part = terms(spot(xx, core, wave))
            acc[at, :, :vd] = value
            acc[at, :, vd:] = rotary_part
            arrive(dd_in.at[at], dd_s.at[at], dd_r.at[at], partner)
            if slot == 0:
                for h, device in ((0, right), (1, left)):
                    opp_out[wave, h] = chip_sum(wave, 0, halves[h]).astype(BF16)
                    k = wave * 2 + h
                    send(opp_out.at[wave, h], opp_in.at[wave, h], op_s.at[k], op_r.at[k], device)
            if slot == 1:
                send_rs(wave, 0, 1, None)
            if slot == 2:
                send_rs(wave, 1, 0, None)

    def send_rs(wave, way, h, extra):
        part = chip_sum(wave, 1 + way, halves[h])
        if extra is not None:
            part = part + extra.astype(F32)
        rs_out[wave, way, h] = part.astype(BF16)
        k = (wave * 2 + way) * 2 + h
        device = (right, left)[way]
        send(rs_out.at[wave, way, h], rs_in.at[wave, way, h], rs_s.at[k], rs_r.at[k], device)

    def relay_wave(wave):
        for h, device in ((0, right), (1, left)):
            k = wave * 2 + h
            arrive(opp_in.at[wave, h], op_s.at[k], op_r.at[k], device)
            send_rs(wave, h, h, opp_in[wave, h])

    gc = gc_ref
    landed = []

    def piece(xx, cc, wave, h):
        at = (xx * 2 + cc) * own_keys + wave * wave_keys + h * half_keys
        return pl.ds(pl.multiple_of(at, half_keys), half_keys)

    def write_out(xx, cc, wave, h):
        at = piece(xx, cc, wave, h)
        k = len(landed)
        copy = pltpu.make_async_copy(full.at[at, :], gc.at[at, :], out_sem.at[k])
        copy.start()
        landed.append(copy)

    full = keys

    def finish_wave(wave):
        for h in range(2):
            for way in range(2):
                k = (wave * 2 + way) * 2 + h
                arrive(rs_in.at[wave, way, h], rs_s.at[k], rs_r.at[k], (right, left)[way])
        for h in range(2):
            done = chip_sum(wave, 3, halves[h])
            done = done + rs_in[wave, 0, h].astype(F32) + rs_in[wave, 1, h].astype(F32)
            full[piece(x, core, wave, h), :] = done.astype(BF16)
        for h, way in ((0, 0), (1, 1), (1, 0), (0, 1)):
            src = full.at[piece(x, core, wave, h), :]
            k = (wave * 2 + way) * 2 + h
            send(src, src, ag_s.at[k], ag_r.at[k], (right, left)[way])
        for h in range(2):
            to_partner(0, x, wave, h)
            write_out(x, core, wave, h)

    def to_partner(kind, xx, wave, h):
        src = full.at[piece(xx, core, wave, h), :]
        k = (kind * 2 + wave) * 2 + h
        send(src, src, pp_s.at[k], pp_r.at[k], partner)

    def from_side(wave, way, h):
        xx = (x + (SX - 1 if way == 0 else 1)) % SX
        here = full.at[piece(xx, core, wave, h), :]
        k = (wave * 2 + way) * 2 + h
        arrive(here, ag_s.at[k], ag_r.at[k], (right, left)[way])
        if h == way:
            k = wave * 2 + way
            send(here, here, fw_s.at[k], fw_r.at[k], (right, left)[way])
        to_partner(1 + way, xx, wave, h)
        write_out(xx, core, wave, h)

    def from_far(wave, way):
        xx = (x + 2) % SX
        here = full.at[piece(xx, core, wave, way), :]
        k = wave * 2 + way
        arrive(here, fw_s.at[k], fw_r.at[k], (right, left)[way])
        to_partner(3, xx, wave, way)
        write_out(xx, core, wave, way)

    def from_partner(wave):
        for kind, offset in enumerate((0, 3, 1, 2)):
            for h in range(2):
                xx = (x + offset) % SX
                here = full.at[piece(xx, 1 - core, wave, h), :]
                k = (kind * 2 + wave) * 2 + h
                arrive(here, pp_s.at[k], pp_r.at[k], partner)
                write_out(xx, 1 - core, wave, h)

    start_wave(0)
    relay_wave(0)
    start_wave(1)

    gq_t = jnp.dot(keys_t[...], grads[...], preferred_element_type=F32)
    gq_out[:, :, :vd] = gq_t[:vd].T.astype(BF16).reshape(CTX, per, vd)
    gq_out[:, :, vd:] = gq_t[vd:].T.astype(BF16).reshape(CTX, per, width - vd)

    def send_gq(k, carry):
        to = (ctx + k) % CTX
        remote(gq_out.at[to], gq_in.at[k], gq_s.at[k], gq_r.at[k], (to, head)).start()
        return carry

    lax.fori_loop(1, CTX, send_gq, 0)

    relay_wave(1)
    finish_wave(0)
    for way in range(2):
        from_side(0, way, way)
    finish_wave(1)
    for way in range(2):
        from_side(0, way, 1 - way)
    for way in range(2):
        from_side(1, way, way)

    def add_att(k, total):
        remote(att_in.at[k], att_in.at[k], at_s.at[k], at_r.at[k], ((ctx + k) % CTX, head)).wait_recv()
        return total + att_in[k].astype(F32)

    att_ref[...] = lax.fori_loop(1, CTX, add_att, att_out[ctx].astype(F32)).astype(BF16)

    def add_gq(k, total):
        remote(gq_in.at[k], gq_in.at[k], gq_s.at[k], gq_r.at[k], ((ctx + k) % CTX, head)).wait_recv()
        return total + gq_in[k].astype(F32)

    grad_query = lax.fori_loop(1, CTX, add_gq, gq_out[ctx].astype(F32))
    rotary = grad_query[:, vd:]
    gq_ref[:, :vd] = grad_query[:, :vd]
    gq_ref[:, vd:] = rotary * cosines - swapped(rotary) * signed

    for way in range(2):
        from_far(0, way)
    for way in range(2):
        from_side(1, way, 1 - way)
    for way in range(2):
        from_far(1, way)
    from_partner(0)
    from_partner(1)

    def drain(k, carry):
        to = (ctx + k) % CTX
        remote(att_out.at[to], att_in.at[k], at_s.at[k], at_r.at[k], (to, head)).wait_send()
        remote(gq_out.at[to], gq_in.at[k], gq_s.at[k], gq_r.at[k], (to, head)).wait_send()
        return carry

    lax.fori_loop(1, CTX, drain, 0)
    for copy in sends:
        copy.wait_send()
    for copy in landed:
        copy.wait()


def rotation_tables(half_width):
    frequency = 10000.0 ** (-np.arange(half_width) / half_width)
    angles = np.outer(2.0 ** np.arange(position_bits), frequency)
    angles = np.concatenate([angles, angles], axis=1)
    return np.cos(angles).astype(np.float32), np.sin(angles).astype(np.float32)


def body(query, cache, cotangent, positions, visible):
    _, per, width = query.shape
    vd = cotangent.shape[-1]
    n_keys = cache.shape[0]
    rows = CTX * per
    wave_keys = n_keys // HEAD // 2
    half_keys = wave_keys // 2
    cos_table, sin_table = rotation_tables((width - vd) // 2)
    vmem = pl.BlockSpec(memory_space=pltpu.VMEM)
    smem = pl.BlockSpec(memory_space=pltpu.SMEM)
    hbm = pl.BlockSpec(memory_space=pl.ANY)
    V, dma = pltpu.VMEM, pltpu.SemaphoreType.DMA
    scratch = [
        V((SZ, SY, per, width), BF16),
        V((SZ, SY, per, vd), BF16),
        V((n_keys, width), BF16),
        V((width, n_keys), BF16),
        V((width, rows), BF16),
        V((vd, rows), BF16),
        V((2 * rows, vd), BF16),
        V((n_keys, rows), F32),
        V((n_keys, rows), F32),
        V((n_keys, rows), BF16),
        V((n_keys, rows), BF16),
        V((16, 128), F32),
        V((SY, 16, 128), F32),
        V((SZ, 16, 128), F32),
        V((8, wave_keys, width), F32),
        V((8, wave_keys, width), BF16),
        V((8, wave_keys, width), BF16),
        V((2, 2, half_keys, width), BF16),
        V((2, 2, half_keys, width), BF16),
        V((2, 2, 2, half_keys, width), BF16),
        V((2, 2, 2, half_keys, width), BF16),
        V((CTX, per, vd), BF16),
        V((CTX, per, vd), BF16),
        V((CTX, per, width), BF16),
        V((CTX, per, width), BF16),
        dma(()),
        dma((SY,)), dma((SY,)), dma((SZ * SY,)), dma((SZ * SY,)),
        dma((SZ,)), dma((SZ,)), dma((SY,)), dma((SY,)),
        dma((SY,)), dma((SY,)), dma((SZ,)), dma((SZ,)),
        dma((8,)), dma((8,)), dma((4,)), dma((4,)), dma((8,)), dma((8,)),
        dma((8,)), dma((8,)), dma((4,)), dma((4,)), dma((16,)), dma((16,)),
        dma((32,)),
        dma((CTX,)), dma((CTX,)), dma((CTX,)), dma((CTX,)),
    ]
    attention, grad_query, grad_cache = pl.pallas_call(
        kernel,
        out_shape=(
            jax.ShapeDtypeStruct((per, vd), BF16),
            jax.ShapeDtypeStruct((per, width), F32),
            jax.ShapeDtypeStruct((n_keys, width), BF16),
        ),
        in_specs=[smem, smem, vmem, vmem, vmem, vmem, hbm],
        out_specs=(vmem, vmem, hbm),
        scratch_shapes=scratch,
        compiler_params=pltpu.CompilerParams(
            collective_id=0, has_side_effects=True, vmem_limit_bytes=62 * 1024 * 1024
        ),
        name="latent_attention",
    )(
        visible,
        positions,
        jnp.asarray(cos_table),
        jnp.asarray(sin_table),
        query.reshape(per, width),
        cotangent.reshape(per, vd),
        cache,
    )
    return attention[None], grad_query[None], grad_cache


def solution(mesh):
    placed = (P("ctx", "head", None), P("ctx", None), P("ctx", "head", None), P("ctx"), P())
    return jax.shard_map(
        body,
        mesh=mesh,
        in_specs=placed,
        out_specs=(P("ctx", "head", None), P("ctx", "head", None), P("ctx", None)),
        check_vma=False,
    )
```

```python
import jax
import jax.numpy as jnp
import numpy as np
from jax import lax
from jax.experimental import pallas as pl
from jax.experimental.pallas import tpu as pltpu
from jax.sharding import PartitionSpec as P

softmax_scale = 192.0 ** (-0.5)
log2_scale = softmax_scale * float(np.log2(np.e))
position_bits = 18
masked_value = -1e30

SZ, SY, SX = 8, 4, 4
CTX, HEAD = SZ * SY, SX * 2
F32, BF16 = jnp.float32, jnp.bfloat16
MESH = pl.DeviceIdType.MESH


def remote(src, dst, send_sem, recv_sem, device):
    return pltpu.make_async_remote_copy(
        src_ref=src,
        dst_ref=dst,
        send_sem=send_sem,
        recv_sem=recv_sem,
        device_id=device,
        device_id_type=MESH,
    )


def dot_nt(a, b):
    return lax.dot_general(a, b, (((1,), (1,)), ((), ())), preferred_element_type=F32)


def kernel(
    vis_ref, pos_ref, cos_ref, sin_ref, query_ref, cot_ref, cache_ref,
    att_ref, gq_ref, gc_ref,
    qb, dob, keys_t, qdo_t, qr_t, scores, gprobs, low,
    seen, seen_f, line_a, line_b, stat_own, stat_y, stat_z, acc, dd_out, dd_in, opp_out, opp_in, rs_out, rs_in,
    att_out, att_in, gq_out, gq_in,
    cache_sem, qy_s, qy_r, qz_s, qz_r, dz_s, dz_r, dy_s, dy_r,
    sy_s, sy_r, sz_s, sz_r, dd_s, dd_r, op_s, op_r, rs_s, rs_r,
    ag_s, ag_r, fw_s, fw_r, pp_s, pp_r, at_s, at_r, gq_s, gq_r,
):
    ctx = lax.axis_index("ctx")
    head = lax.axis_index("head")
    z, y = ctx // SY, ctx % SY
    x, core = head // 2, head % 2
    n_keys = keys_t.shape[1]
    vd = cot_ref.shape[2]
    width = query_ref.shape[2]
    per = query_ref.shape[1]
    rows = CTX * per
    own_keys = n_keys // HEAD
    wave_keys = own_keys // 2
    half_keys = wave_keys // 2
    sends = []

    def plane(zz, yy):
        return (zz % SZ) * SY + yy % SY, head

    right = (ctx, ((x + 1) % SX) * 2 + core)
    left = (ctx, ((x + SX - 1) % SX) * 2 + core)
    partner = (ctx, x * 2 + 1 - core)

    def send(*args):
        copy = remote(*args)
        copy.start()
        sends.append(copy)

    def arrive(dst, send_sem, recv_sem, device):
        remote(dst, dst, send_sem, recv_sem, device).wait_recv()

    load = pltpu.make_async_copy(cache_ref, keys_t, cache_sem)
    load.start()

    barrier = pltpu.get_barrier_semaphore()

    def greet(k, carry):
        pl.semaphore_signal(
            barrier, inc=1, device_id=((ctx + k) % CTX, head), device_id_type=MESH
        )
        return carry

    lax.fori_loop(1, CTX, greet, 0)
    for device in (right, left, partner):
        pl.semaphore_signal(barrier, inc=1, device_id=device, device_id_type=MESH)

    position = pos_ref[0]
    half = (width - vd) // 2
    cosines = jnp.ones((1, 2 * half), F32)
    sines = jnp.zeros((1, 2 * half), F32)
    for bit in range(position_bits):
        switch = ((position >> bit) & 1).astype(F32)
        step_cos = 1.0 + switch * (cos_ref[bit : bit + 1, :] - 1.0)
        step_sin = switch * sin_ref[bit : bit + 1, :]
        cosines, sines = (
            cosines * step_cos - sines * step_sin,
            sines * step_cos + cosines * step_sin,
        )
    lower = lax.broadcasted_iota(jnp.int32, (1, 2 * half), 1) < half
    signed = jnp.where(lower, -sines, sines)

    def swapped(t):
        return jnp.concatenate([t[:, half:], t[:, :half]], axis=1)

    rotary = query_ref[0, :, vd:].astype(F32)
    qb[z, y, :, :vd] = query_ref[0, :, :vd]
    qb[z, y, :, vd:] = (rotary * cosines + swapped(rotary) * signed).astype(BF16)
    dob[z, y] = cot_ref[0]

    for t in range(CTX):
        seen[t * per : (t + 1) * per, :] = jnp.full((per, 128), vis_ref[t], jnp.int32)

    pl.semaphore_wait(barrier, CTX - 1 + 3)

    for d in range(1, SY):
        send(qb.at[z, y], qb.at[z, y], qy_s.at[d], qy_r.at[d], plane(z, y + d))
    for d in range(1, SZ):
        send(dob.at[z, y], dob.at[z, y], dz_s.at[d], dz_r.at[d], plane(z + d, y))

    def ring(way, step, d):
        sign = 1 if way == 0 else -1
        zz = (z - sign * (step - 1) + SZ) % SZ
        yy = (y - d + SY) % SY
        at = (way * (SZ // 2) + step - 1) * SY + d
        block = qb.at[zz, yy]
        send(block, block, qz_s.at[at], qz_r.at[at], plane(z + sign + SZ, y))

    def ring_arrive(way, step, d):
        sign = 1 if way == 0 else -1
        zz = (z - sign * step + SZ) % SZ
        yy = (y - d + SY) % SY
        at = (way * (SZ // 2) + step - 1) * SY + d
        arrive(qb.at[zz, yy], qz_s.at[at], qz_r.at[at], plane(z + sign + SZ, y))

    def carried(way, step, d):
        return step < SZ // 2 or (d < SY // 2) == (way == 0)

    for d in range(SY):
        if d:
            src = qb.at[z, (y - d + SY) % SY]
            arrive(src, qy_s.at[d], qy_r.at[d], plane(z, y + d))
        ring(0, 1, d)
        ring(1, 1, d)
    for step in range(1, SZ // 2 + 1):
        for d in range(SY):
            for way in range(2):
                if carried(way, step, d):
                    ring_arrive(way, step, d)
                    if step < SZ // 2 and carried(way, step + 1, d):
                        ring(way, step + 1, d)
        if step == 2:
            for d in range(1, SZ):
                src = dob.at[(z - d + SZ) % SZ, y]
                arrive(src, dz_s.at[d], dz_r.at[d], plane(z + d, y))
            for d in range(1, SY):
                src = dob.at[:, y]
                send(src, src, dy_s.at[d], dy_r.at[d], plane(z, y + d))

    load.wait()
    chunk = 256
    n_chunks = n_keys // chunk
    first_key = ctx * n_keys
    line_a[...] = jnp.full(line_a.shape, 2 * masked_value, F32)

    def score(i, carry):
        at = pl.multiple_of(i * chunk, chunk)
        raw = jnp.dot(
            qb[...].reshape(rows, width), keys_t[:, pl.ds(at, chunk)], preferred_element_type=F32
        )
        top = line_a[...]
        for part in range(chunk // 128):
            spot_at = pl.multiple_of(at + part * 128, 128)
            piece = raw[:, part * 128 : (part + 1) * 128] * log2_scale
            piece = jnp.where(first_key + spot_at < seen[...], piece, masked_value)
            scores[:, pl.ds(spot_at, 128)] = piece
            top = jnp.maximum(top, piece)
        line_a[...] = top
        return carry

    lax.fori_loop(0, n_chunks, score, 0)
    peak = jnp.max(line_a[...], axis=1, keepdims=True)
    peak_line = line_b
    peak_line[...] = jnp.broadcast_to(peak, peak_line.shape)

    for d in range(1, SY):
        src = dob.at[:, (y - d + SY) % SY]
        arrive(src, dy_s.at[d], dy_r.at[d], plane(z, y + d))

    mass_line, inner_line = line_a, seen_f
    mass_line[...] = jnp.zeros(line_a.shape, F32)
    inner_line[...] = jnp.zeros(line_a.shape, F32)

    def weigh(i, carry):
        at = pl.multiple_of(i * chunk, chunk)
        gp = jnp.dot(
            dob[...].reshape(rows, vd), keys_t[:vd, pl.ds(at, chunk)], preferred_element_type=F32
        )
        gprobs[:, pl.ds(at, chunk)] = gp
        mass, inner = mass_line[...], inner_line[...]
        for part in range(chunk // 128):
            window = pl.ds(pl.multiple_of(at + part * 128, 128), 128)
            weights = jnp.exp2(scores[:, window] - peak_line[...])
            scores[:, window] = weights
            low[:, window] = weights.astype(BF16)
            mass = mass + weights
            inner = inner + weights * gp[:, part * 128 : (part + 1) * 128]
        mass_line[...] = mass
        inner_line[...] = inner
        return carry

    lax.fori_loop(0, n_chunks, weigh, 0)
    mass = jnp.sum(mass_line[...], axis=1, keepdims=True)
    inner = jnp.sum(inner_line[...], axis=1, keepdims=True)
    lanes = lax.broadcasted_iota(jnp.int32, (rows, 128), 1)
    table = jnp.where(lanes == 0, peak, jnp.where(lanes == 1, mass, inner)).T
    peak, mass, inner = (table[i : i + 1, :] for i in range(3))

    n_lines = rows // 128

    def put_stats(ref, stats):
        for k, stat in enumerate(stats):
            for i in range(n_lines):
                ref[k * n_lines + i : k * n_lines + i + 1, :] = stat[:, i * 128 : (i + 1) * 128]

    def merge(parts):
        tops = [p[:n_lines] for p in parts]
        best = tops[0]
        for t in tops[1:]:
            best = jnp.maximum(best, t)
        total, dots = 0.0, 0.0
        for t, p in zip(tops, parts):
            factor = jnp.exp2(t - best)
            total = total + factor * p[n_lines : 2 * n_lines]
            dots = dots + factor * p[2 * n_lines : 3 * n_lines]
        return best, total, dots

    put_stats(stat_own, (peak, mass, inner, jnp.zeros_like(peak)))
    for d in range(1, SY):
        send(stat_own, stat_y.at[d], sy_s.at[d], sy_r.at[d], plane(z, y + d))
    first = dot_nt(low[: rows // 2, :], keys_t[:vd, :])
    for d in range(1, SY):
        arrive(stat_y.at[d], sy_s.at[d], sy_r.at[d], plane(z, y + d))
    best, total, dots = merge([stat_own[...]] + [stat_y[d] for d in range(1, SY)])
    stat_z[0, :n_lines] = best
    stat_z[0, n_lines : 2 * n_lines] = total
    stat_z[0, 2 * n_lines : 3 * n_lines] = dots
    stat_z[0, 3 * n_lines :] = jnp.zeros_like(dots)
    for d in range(1, SZ):
        send(stat_z.at[0], stat_z.at[d], sz_s.at[d], sz_r.at[d], plane(z + d, y))
    second = dot_nt(low[rows // 2 :, :], keys_t[:vd, :])
    attended = jnp.concatenate([first, second], axis=0)
    q_all = qb[...].reshape(rows, width)
    qdo_t[:, :rows] = q_all[:, :vd].T
    qdo_t[:, rows:] = dob[...].reshape(rows, vd).T
    qr_t[...] = q_all[:, vd:].T
    for d in range(1, SZ):
        arrive(stat_z.at[d], sz_s.at[d], sz_r.at[d], plane(z + d, y))
    best, total, dots = merge([stat_z[d] for d in range(SZ)])

    def across(v):
        return jnp.concatenate([v[i : i + 1, :] for i in range(n_lines)], axis=1)

    def down(v):
        return jnp.broadcast_to(v, (128, rows)).T

    factor, delta = line_a, line_b
    factor[...] = down(jnp.exp2(peak - across(best)) / across(total))
    delta[...] = down(across(dots) / across(total))

    for i in range(vd // 128):
        cols = slice(i * 128, (i + 1) * 128)
        block = attended[:, cols] * factor[...]
        att_out[:, :, cols] = block.astype(BF16).reshape(CTX, per, 128)

    def send_att(k, carry):
        to = (ctx + k) % CTX
        remote(att_out.at[to], att_in.at[k], at_s.at[k], at_r.at[k], (to, head)).start()
        return carry

    def spot(xx, cc, wave):
        return pl.multiple_of((xx * 2 + cc) * own_keys + wave * wave_keys, wave_keys)

    def terms(at):
        grad, probs = [], []
        for part in range(wave_keys // 128):
            window = pl.ds(pl.multiple_of(at + part * 128, 128), 128)
            prob = scores[:, window] * factor[...]
            grad.append((prob * (gprobs[:, window] - delta[...]) * softmax_scale).astype(BF16))
            probs.append(prob.astype(BF16))
        grad = jnp.concatenate(grad, axis=1)
        low[:, pl.ds(at, wave_keys)] = grad
        both = jnp.concatenate([grad, jnp.concatenate(probs, axis=1)], axis=0)
        value = jnp.dot(qdo_t[...], both, preferred_element_type=F32)
        return value, jnp.dot(qr_t[...], grad, preferred_element_type=F32)

    offsets = (2, 1, 3, 0)
    halves = (slice(0, half_keys), slice(half_keys, 2 * half_keys))

    def chip_sum(wave, slot, part):
        at = wave * 4 + slot
        return acc[at, :, part] + dd_in[at, :, part].astype(F32)

    def start_wave(wave):
        for slot, offset in enumerate(offsets):
            if slot == 3:
                relay_wave(wave)
            at = wave * 4 + slot
            xx = (x + offset) % SX
            value, rotary_part = terms(spot(xx, 1 - core, wave))
            dd_out[at, :vd, :] = value.astype(BF16)
            dd_out[at, vd:, :] = rotary_part.astype(BF16)
            send(dd_out.at[at], dd_in.at[at], dd_s.at[at], dd_r.at[at], partner)
            value, rotary_part = terms(spot(xx, core, wave))
            acc[at, :vd, :] = value
            acc[at, vd:, :] = rotary_part
            arrive(dd_in.at[at], dd_s.at[at], dd_r.at[at], partner)
            if slot == 0:
                if wave == 0:
                    lax.fori_loop(1, CTX, send_att, 0)
                for h, device in ((0, right), (1, left)):
                    opp_out[wave, h] = chip_sum(wave, 0, halves[h]).astype(BF16)
                    k = wave * 2 + h
                    send(opp_out.at[wave, h], opp_in.at[wave, h], op_s.at[k], op_r.at[k], device)
            if slot == 1:
                send_rs(wave, 0, 1, None)
            if slot == 2:
                send_rs(wave, 1, 0, None)

    def send_rs(wave, way, h, extra):
        part = chip_sum(wave, 1 + way, halves[h])
        if extra is not None:
            part = part + extra.astype(F32)
        rs_out[wave, way, h] = part.astype(BF16)
        k = (wave * 2 + way) * 2 + h
        device = (right, left)[way]
        send(rs_out.at[wave, way, h], rs_in.at[wave, way, h], rs_s.at[k], rs_r.at[k], device)

    def relay_wave(wave):
        for h, device in ((0, right), (1, left)):
            k = wave * 2 + h
            arrive(opp_in.at[wave, h], op_s.at[k], op_r.at[k], device)
            send_rs(wave, h, h, opp_in[wave, h])

    full = gc_ref

    def piece(xx, cc, wave, h):
        return (xx * 2 + cc) * 4 + wave * 2 + h

    def finish_wave(wave):
        for h in range(2):
            for way in range(2):
                k = (wave * 2 + way) * 2 + h
                arrive(rs_in.at[wave, way, h], rs_s.at[k], rs_r.at[k], (right, left)[way])
        for h in range(2):
            done = chip_sum(wave, 3, halves[h])
            done = done + rs_in[wave, 0, h].astype(F32) + rs_in[wave, 1, h].astype(F32)
            full[piece(x, core, wave, h)] = done.astype(BF16)
        for h, way in ((0, 0), (1, 1), (1, 0), (0, 1)):
            src = full.at[piece(x, core, wave, h)]
            k = (wave * 2 + way) * 2 + h
            send(src, src, ag_s.at[k], ag_r.at[k], (right, left)[way])
        for h in range(2):
            to_partner(0, x, wave, h)

    def to_partner(kind, xx, wave, h):
        src = full.at[piece(xx, core, wave, h)]
        k = (kind * 2 + wave) * 2 + h
        send(src, src, pp_s.at[k], pp_r.at[k], partner)

    def from_side(wave, way, h):
        xx = (x + (SX - 1 if way == 0 else 1)) % SX
        here = full.at[piece(xx, core, wave, h)]
        k = (wave * 2 + way) * 2 + h
        arrive(here, ag_s.at[k], ag_r.at[k], (right, left)[way])
        if h == way:
            k = wave * 2 + way
            send(here, here, fw_s.at[k], fw_r.at[k], (right, left)[way])
        to_partner(1 + way, xx, wave, h)

    def from_far(wave, way):
        xx = (x + 2) % SX
        here = full.at[piece(xx, core, wave, way)]
        k = wave * 2 + way
        arrive(here, fw_s.at[k], fw_r.at[k], (right, left)[way])
        to_partner(3, xx, wave, way)

    def from_partner(wave):
        for kind, offset in enumerate((0, 3, 1, 2)):
            for h in range(2):
                xx = (x + offset) % SX
                here = full.at[piece(xx, 1 - core, wave, h)]
                k = (kind * 2 + wave) * 2 + h
                arrive(here, pp_s.at[k], pp_r.at[k], partner)

    start_wave(0)
    start_wave(1)
    finish_wave(0)

    grad_rotated = dot_nt(low[...], keys_t[...])
    gq_out[...] = grad_rotated.astype(BF16).reshape(CTX, per, width)

    def send_gq(k, carry):
        to = (ctx + k) % CTX
        remote(gq_out.at[to], gq_in.at[k], gq_s.at[k], gq_r.at[k], (to, head)).start()
        return carry

    lax.fori_loop(1, CTX, send_gq, 0)

    for way in range(2):
        from_side(0, way, way)
    finish_wave(1)
    for way in range(2):
        from_side(0, way, 1 - way)
    for way in range(2):
        from_side(1, way, way)

    def add_att(k, total):
        remote(att_in.at[k], att_in.at[k], at_s.at[k], at_r.at[k], ((ctx + k) % CTX, head)).wait_recv()
        return total + att_in[k].astype(F32)

    att_ref[0] = lax.fori_loop(1, CTX, add_att, att_out[ctx].astype(F32)).astype(BF16)

    def add_gq(k, total):
        remote(gq_in.at[k], gq_in.at[k], gq_s.at[k], gq_r.at[k], ((ctx + k) % CTX, head)).wait_recv()
        return total + gq_in[k].astype(F32)

    grad_query = lax.fori_loop(1, CTX, add_gq, gq_out[ctx].astype(F32))
    rotary = grad_query[:, vd:]
    gq_ref[0, :, :vd] = grad_query[:, :vd]
    gq_ref[0, :, vd:] = rotary * cosines - swapped(rotary) * signed

    for way in range(2):
        from_far(0, way)
    for way in range(2):
        from_side(1, way, 1 - way)
    for way in range(2):
        from_far(1, way)
    from_partner(0)
    from_partner(1)

    def drain(k, carry):
        to = (ctx + k) % CTX
        remote(att_out.at[to], att_in.at[k], at_s.at[k], at_r.at[k], (to, head)).wait_send()
        remote(gq_out.at[to], gq_in.at[k], gq_s.at[k], gq_r.at[k], (to, head)).wait_send()
        return carry

    lax.fori_loop(1, CTX, drain, 0)
    for copy in sends:
        copy.wait_send()


def put_out(att_held, gq_held, gc_held, att_ref, gq_ref, gc_ref, sems):
    pieces = gc_held.shape[0]
    copies = [
        pltpu.make_async_copy(gc_held.at[i], gc_ref.at[:, i * 128 : (i + 1) * 128], sems.at[i])
        for i in range(pieces)
    ]
    copies.append(pltpu.make_async_copy(att_held, att_ref, sems.at[pieces]))
    copies.append(pltpu.make_async_copy(gq_held, gq_ref, sems.at[pieces + 1]))
    for copy in copies:
        copy.start()
    for copy in copies:
        copy.wait()


def rotation_tables(half_width):
    frequency = 10000.0 ** (-np.arange(half_width) / half_width)
    angles = np.outer(2.0 ** np.arange(position_bits), frequency)
    angles = np.concatenate([angles, angles], axis=1)
    return np.cos(angles).astype(np.float32), np.sin(angles).astype(np.float32)


def body(query, cache, cotangent, positions, visible):
    _, per, width = query.shape
    vd = cotangent.shape[-1]
    n_keys = cache.shape[0]
    rows = CTX * per
    wave_keys = n_keys // HEAD // 2
    half_keys = wave_keys // 2
    cos_table, sin_table = rotation_tables((width - vd) // 2)
    vmem = pl.BlockSpec(memory_space=pltpu.VMEM)
    smem = pl.BlockSpec(memory_space=pltpu.SMEM)
    hbm = pl.BlockSpec(memory_space=pl.ANY)
    V, dma = pltpu.VMEM, pltpu.SemaphoreType.DMA
    scratch = [
        V((SZ, SY, per, width), BF16),
        V((SZ, SY, per, vd), BF16),
        V((width, n_keys), BF16),
        V((vd, 2 * rows), BF16),
        V((width - vd, rows), BF16),
        V((rows, n_keys), F32),
        V((rows, n_keys), F32),
        V((rows, n_keys), BF16),
        V((rows, 128), jnp.int32),
        V((rows, 128), F32),
        V((rows, 128), F32),
        V((rows, 128), F32),
        V((16, 128), F32),
        V((SY, 16, 128), F32),
        V((SZ, 16, 128), F32),
        V((8, width, wave_keys), F32),
        V((8, width, wave_keys), BF16),
        V((8, width, wave_keys), BF16),
        V((2, 2, width, half_keys), BF16),
        V((2, 2, width, half_keys), BF16),
        V((2, 2, 2, width, half_keys), BF16),
        V((2, 2, 2, width, half_keys), BF16),
        V((CTX, per, vd), BF16),
        V((CTX, per, vd), BF16),
        V((CTX, per, width), BF16),
        V((CTX, per, width), BF16),
        dma(()),
        dma((SY,)), dma((SY,)), dma((SZ * SY,)), dma((SZ * SY,)),
        dma((SZ,)), dma((SZ,)), dma((SY,)), dma((SY,)),
        dma((SY,)), dma((SY,)), dma((SZ,)), dma((SZ,)),
        dma((8,)), dma((8,)), dma((4,)), dma((4,)), dma((8,)), dma((8,)),
        dma((8,)), dma((8,)), dma((4,)), dma((4,)), dma((16,)), dma((16,)),
        dma((CTX,)), dma((CTX,)), dma((CTX,)), dma((CTX,)),
    ]
    pieces = n_keys // 128
    held = (
        V((1, per, vd), BF16),
        V((1, per, width), F32),
        V((pieces, width, 128), BF16),
    )
    held = pl.pallas_call(
        kernel,
        out_shape=held,
        in_specs=[smem, smem, vmem, vmem, vmem, vmem, hbm],
        out_specs=(vmem, vmem, vmem),
        scratch_shapes=scratch,
        compiler_params=pltpu.CompilerParams(
            collective_id=0, has_side_effects=True, vmem_limit_bytes=56 * 1024 * 1024
        ),
        name="latent_attention",
    )(
        visible,
        positions,
        jnp.asarray(cos_table),
        jnp.asarray(sin_table),
        query,
        cotangent,
        cache.T,
    )
    attention, grad_query, grad_cache = pl.pallas_call(
        put_out,
        out_shape=(
            jax.ShapeDtypeStruct((1, per, vd), BF16),
            jax.ShapeDtypeStruct((1, per, width), F32),
            jax.ShapeDtypeStruct((width, n_keys), BF16),
        ),
        in_specs=[hbm, hbm, hbm],
        out_specs=(hbm, hbm, hbm),
        scratch_shapes=[dma((pieces + 2,))],
        compiler_params=pltpu.CompilerParams(vmem_limit_bytes=1024 * 1024),
        name="put_out",
    )(*held)
    return attention, grad_query, grad_cache.T


def solution(mesh):
    placed = (P("ctx", "head", None), P("ctx", None), P("ctx", "head", None), P("ctx"), P())
    return jax.shard_map(
        body,
        mesh=mesh,
        in_specs=placed,
        out_specs=(P("ctx", "head", None), P("ctx", "head", None), P("ctx", None)),
        check_vma=False,
    )
```
